128 devices in a mesh: along: 32 (over x, y, core), across: 4 (over z).
Axes of the slice: x: 4, y: 4, z: 4, core: 2. Of those that a mesh axis runs over, the one named last changes fastest.
Arguments:
- fields: float32 [40, 3, 32, 16384], P(None, None, 'across', 'along'), may hold values from -6 to 6
- first_feet: int32 [32, 16384], P('across', 'along'), may hold values from 0 to 524287, as said below
- first_fraction: float32 [40, 32, 16384], P(None, 'across', 'along'), may hold values from 0 to 1
- second_feet: int32 [32, 16384], P('across', 'along'), may hold values from 0 to 524287, as said below
- second_fraction: float32 [40, 32, 16384], P(None, 'across', 'along'), may hold values from 0 to 1
- lateral_mix: float32 [32, 16384], P('across', 'along'), may hold values from 0.02 to 0.2
- vertical_mix: float32 [2, 39, 32, 16384], P(None, None, 'across', 'along'), may hold values from 0.05 to 5
- bottom_drag: float32 [32, 16384], P('across', 'along'), may hold values from 0.05 to 2
- surface_stress: float32 [2, 32, 16384], P(None, 'across', 'along'), may hold values from -3 to 3
Outputs:
- advanced: float32 [40, 3, 32, 16384], P(None, None, 'across', 'along')
The draws below stay inside these ranges and needn't reach their ends.
Inputs may be any that keep to these rules, and one draw needn't show every extreme that they name: `first_feet`: A cell in the block of 8 x 512 cells with along block index a has its foot point (row p // 16384, column p % 16384) in a block whose along index lies from w to w + 3, w = max(a - 3, 0), at any cross block index. At most 288 cells of one block have foot points in one block, and some pair of blocks reaches 288. `second_feet`: as for first_feet.
All inputs are finite; a program needn't handle non-finite values.
Results may differ from the reference program's by a relative error of at most 0.00002.
Values sent between devices are 32-bit elements; how exact they have to be, the bound alone decides.
No kernel may reach another device: no remote copies, remote signals or barrier semaphores. Data moves between devices by JAX's collectives and lax.ppermute only.
A program may use at most 64 MiB of HBM per device.

```python
import math
import jax
import jax.numpy as jnp

LAYERS = 40
CROSS_DEV = 8
ALONG_DEV = 512
REACH = 4
CAPACITY = 288
CELLS_ACROSS = 32
CELLS_ALONG = 16384


def make_feet(key):
    along_count = CELLS_ALONG // ALONG_DEV
    across_count = CELLS_ACROSS // CROSS_DEV
    cells_dev = CROSS_DEV * ALONG_DEV
    partners = across_count * REACH
    slot_total = partners * CAPACITY
    subkeys = jax.random.split(key, 6)
    hot_along = jax.random.randint(subkeys[0], (), 0, along_count)
    hot_across = jax.random.randint(subkeys[1], (), 0, across_count)
    window = jnp.maximum(jnp.arange(along_count) - REACH + 1, 0)
    has_hot = (hot_along >= window) & (hot_along < window + REACH)
    hot_slot = (hot_along - window) * across_count + hot_across
    random_slot = jax.random.randint(subkeys[2], (across_count, along_count), 0, partners)
    full_slot = jnp.where(has_hot[None, :], hot_slot[None, :], random_slot)
    labels = jnp.arange(slot_total) // CAPACITY
    scores = jax.random.randint(subkeys[3], (across_count, along_count, slot_total), 0, 4096) * slot_total + jnp.arange(slot_total)
    scores = jnp.where(labels == full_slot[..., None], jnp.arange(slot_total) - slot_total, scores)
    chosen = labels[jnp.argsort(scores, axis=-1)[..., :cells_dev]]
    shuffle = jax.random.randint(subkeys[4], (across_count, along_count, cells_dev), 0, 4096) * cells_dev + jnp.arange(cells_dev)
    chosen = jnp.take_along_axis(chosen, jnp.argsort(shuffle, axis=-1), axis=-1)
    owner_along = window[None, :, None] + chosen // across_count
    owner_across = chosen % across_count
    local_cell = jax.random.randint(subkeys[5], (across_count, along_count, cells_dev), 0, cells_dev)
    global_id = (owner_across * CROSS_DEV + local_cell // ALONG_DEV) * CELLS_ALONG + owner_along * ALONG_DEV + local_cell % ALONG_DEV
    arranged = global_id.reshape(across_count, along_count, CROSS_DEV, ALONG_DEV).transpose(0, 2, 1, 3)
    return arranged.reshape(CELLS_ACROSS, CELLS_ALONG).astype(jnp.int32)


def draw_first_feet(key, part):
    return make_feet(jax.random.fold_in(key, 11))


def draw_second_feet(key, part):
    return make_feet(jax.random.fold_in(key, 23))


def block_levels(stream_key, shape, cuts, smallest, high):
    gain, own = 1.0, jax.random.fold_in(stream_key, 6)
    for dim, blocks in cuts:
        steps = jnp.exp(jax.random.uniform(jax.random.fold_in(own, dim), (blocks,), jnp.float32, smallest / len(cuts), high / len(cuts)))
        gain = gain * jnp.repeat(steps, shape[dim] // blocks).reshape([-1 if axis == dim else 1 for axis in range(len(shape))])
    return gain


def scatter_about(stream_key, dims, deviation, bound, cuts=(), kind=jnp.bfloat16):
    gain = block_levels(stream_key, dims, cuts, -0.22, 0.18) if cuts else 1.0
    values = jax.random.normal(stream_key, dims, jnp.float32) * deviation * gain
    return jnp.minimum(jnp.maximum(values, -bound), bound).astype(kind)


def setup_inputs(seed: int = 0) -> dict:
    streams_of = jax.random.split(jax.random.key(seed), 10)
    return {
        "fields": scatter_about(streams_of[0], (LAYERS, 3, CELLS_ACROSS, CELLS_ALONG), 1.0, 6.0, ((2, 4), (3, 32)), jnp.float32),
        "first_feet": draw_first_feet(jax.random.fold_in(streams_of[9], 71), 0),
        "first_fraction": jnp.clip(1.0 * jax.random.uniform(streams_of[2], (LAYERS, CELLS_ACROSS, CELLS_ALONG), jnp.float32) ** block_levels(streams_of[2], (LAYERS, CELLS_ACROSS, CELLS_ALONG), ((1, 4), (2, 32)), -0.2, 0.2), 0.0, 1.0),
        "second_feet": draw_second_feet(jax.random.fold_in(streams_of[9], 71), 0),
        "second_fraction": jnp.clip(1.0 * jax.random.uniform(streams_of[4], (LAYERS, CELLS_ACROSS, CELLS_ALONG), jnp.float32) ** block_levels(streams_of[4], (LAYERS, CELLS_ACROSS, CELLS_ALONG), ((1, 4), (2, 32)), -0.2, 0.2), 0.0, 1.0),
        "lateral_mix": jnp.clip(jnp.exp(math.log(0.2) - 2.3025851 * jax.random.uniform(streams_of[5], (CELLS_ACROSS, CELLS_ALONG), jnp.float32) ** block_levels(streams_of[5], (CELLS_ACROSS, CELLS_ALONG), ((0, 4), (1, 32)), -0.2, 0.2)), 0.02, 0.2),
        "vertical_mix": jnp.clip(jnp.exp(math.log(5.0) - 4.6051702 * jax.random.uniform(streams_of[6], (2, LAYERS - 1, CELLS_ACROSS, CELLS_ALONG), jnp.float32) ** block_levels(streams_of[6], (2, LAYERS - 1, CELLS_ACROSS, CELLS_ALONG), ((2, 4), (3, 32)), -0.2, 0.2)), 0.05, 5.0),
        "bottom_drag": jnp.clip(jnp.exp(math.log(2.0) - 3.6888794 * jax.random.uniform(streams_of[7], (CELLS_ACROSS, CELLS_ALONG), jnp.float32) ** block_levels(streams_of[7], (CELLS_ACROSS, CELLS_ALONG), ((0, 4), (1, 32)), -0.2, 0.2)), 0.05, 2.0),
        "surface_stress": scatter_about(streams_of[8], (2, CELLS_ACROSS, CELLS_ALONG), 0.5, 3.0, ((1, 4), (2, 32)), jnp.float32),
    }


def interpolate(columns, fraction):
    upper = jnp.concatenate([columns[1:], columns[-1:]], axis=0)
    weight = fraction[:, None]
    return (1.0 - weight) * columns + weight * upper


def neighbour_sum(padded):
    total = padded[:, :, :-2, 1:-1] + padded[:, :, 2:, 1:-1]
    return total + padded[:, :, 1:-1, :-2] + padded[:, :, 1:-1, 2:]


def solve_columns(forcing, vertical_mix, bottom_drag, surface_stress):
    layers = forcing.shape[0]
    coupling = jnp.stack([vertical_mix[0], vertical_mix[0], vertical_mix[1]], axis=1)
    nothing = jnp.zeros_like(coupling[:1])
    below = jnp.concatenate([nothing, coupling], axis=0)
    above = jnp.concatenate([coupling, nothing], axis=0)
    friction = jnp.stack([bottom_drag, bottom_drag, jnp.zeros_like(bottom_drag)], axis=0)
    diagonal = (1.0 + below + above).at[0].add(friction)
    source = forcing.at[layers - 1, 0:2].add(surface_stress)
    factor = above[0] / diagonal[0]
    partial_value = source[0] / diagonal[0]
    factors = [factor]
    partials = [partial_value]
    for level_index in range(1, layers):
        denominator = diagonal[level_index] - below[level_index] * factor
        factor = above[level_index] / denominator
        partial_value = (source[level_index] + below[level_index] * partial_value) / denominator
        factors.append(factor)
        partials.append(partial_value)
    solution = partials[layers - 1]
    results = [solution]
    for level_index in range(layers - 2, -1, -1):
        solution = partials[level_index] + factors[level_index] * solution
        results.append(solution)
    return jnp.stack(results[::-1], axis=0)


def reference(fields, first_feet, first_fraction, second_feet, second_fraction, lateral_mix, vertical_mix, bottom_drag, surface_stress):
    layers, components, row_total, column_total = fields.shape

    def advect(current, feet, fraction):
        flattened = current.reshape(layers * components, row_total * column_total)
        gathered = jnp.take(flattened, feet.reshape(-1).astype(jnp.int32), axis=1)
        return interpolate(gathered.reshape(layers, components, row_total, column_total), fraction)

    middle = advect(fields, first_feet, first_fraction)
    moved = advect(middle, second_feet, second_fraction)
    padded = jnp.pad(moved, ((0, 0), (0, 0), (1, 1), (1, 1)))
    beside_all = neighbour_sum(padded)
    row_index = jnp.arange(row_total, dtype=jnp.int32)
    column_index = jnp.arange(column_total, dtype=jnp.int32)
    row_count = (row_index > 0).astype(jnp.float32) + (row_index < row_total - 1).astype(jnp.float32)
    column_count = (column_index > 0).astype(jnp.float32) + (column_index < column_total - 1).astype(jnp.float32)
    present = row_count[:, None] + column_count[None, :]
    mixed = moved + lateral_mix * (beside_all - present * moved)
    return solve_columns(mixed, vertical_mix, bottom_drag, surface_stress)
```

```python
import functools

import jax
import jax.numpy as jnp
from jax import lax
from jax.experimental import pallas as pl
from jax.experimental.pallas import tpu as pltpu
from jax.sharding import PartitionSpec as P

LAYERS = 40
ROWS = 8
COLS = 512
CELLS = ROWS * COLS
SLOTS = 288
SPAN = 4
WIDE = 128
CHUNKS = COLS // WIDE
LEVELS = 3 * LAYERS
F32 = jnp.float32
I32 = jnp.int32
VMEM = pl.BlockSpec(memory_space=pltpu.VMEM)
SMEM = pl.BlockSpec(memory_space=pltpu.SMEM)


def iota(shape, dim):
    return lax.broadcasted_iota(I32, shape, dim)


def kernel_call(body, out_shapes, in_specs, out_specs, operands, flops=1 << 20, grid=None, scratch=(), name=None):
    extra = {} if grid is None else {"grid": grid}
    return pl.pallas_call(
        body,
        out_shape=out_shapes,
        in_specs=in_specs,
        out_specs=out_specs,
        scratch_shapes=list(scratch),
        cost_estimate=pl.CostEstimate(flops=flops, bytes_accessed=1 << 21, transcendentals=0),
        name=name,
        **extra,
    )(*operands)


def slots_body(along_ref, first_ref, second_ref, wanted_ref, own_ref):
    along = along_ref[0]
    before = (iota((COLS, COLS), 0) < iota((COLS, COLS), 1)).astype(jnp.bfloat16)
    partner_rows = iota((16, COLS), 0)
    slot_rows = iota((128, COLS), 0)
    lane_rows = iota((WIDE, COLS), 0)
    lane = iota((1, COLS), 1)
    total = jnp.zeros((512, WIDE), F32)
    for which, feet_ref in enumerate((first_ref, second_ref)):
        carry = jnp.zeros((16, 1), F32)
        for row in range(ROWS):
            feet = feet_ref[row : row + 1, :]
            global_row = feet >> 14
            column = feet & 16383
            across = global_row >> 3
            owner = column >> 9
            local = (global_row & 7) * COLS + (column & 511)
            kind = jnp.where(owner <= along, along - owner, owner)
            partner = across * SPAN + kind
            mask = partner_rows == partner
            ones = mask.astype(F32)
            prefix = jnp.dot(ones.astype(jnp.bfloat16), before, preferred_element_type=F32)
            rank = jnp.sum(jnp.where(mask, prefix + carry, 0.0), axis=0, keepdims=True).astype(I32)
            carry = carry + jnp.sum(ones, axis=1, keepdims=True)
            slot_row = partner * 8 + which * 3 + (rank >> 7)
            hit = slot_rows == slot_row
            place = (lane_rows == (rank & 127)).astype(F32).astype(jnp.bfloat16)
            own = CELLS - (row * COLS + lane)
            values = []
            for value in (local & 63, local >> 6, own & 63, own >> 6):
                values.append(jnp.where(hit, value.astype(F32), 0.0).astype(jnp.bfloat16))
            total = total + lax.dot_general(
                jnp.concatenate(values, axis=0),
                place,
                (((1,), (1,)), ((), ())),
                preferred_element_type=F32,
            )
    whole = total.astype(I32)
    wanted_ref[...] = whole[0:128] + whole[128:256] * 64
    own_ref[...] = CELLS - (whole[256:384] + whole[384:512] * 64)


def table_body(copies, x_ref, o_ref):
    for row in range(ROWS):
        if copies == 1:
            parts = [x_ref[pl.ds(m * 8 + row, LAYERS, stride=24), :] for m in range(3)]
        else:
            part = x_ref[pl.ds(row, LAYERS, stride=8), :]
            parts = [part, part, part]
        parts.append(jnp.zeros((WIDE - LEVELS, WIDE), F32))
        o_ref[row] = jnp.concatenate(parts, axis=0).T


def cells_first(x, copies):
    rows = x.shape[0]
    return kernel_call(
        functools.partial(table_body, copies),
        jax.ShapeDtypeStruct((ROWS, COLS, WIDE), F32),
        [pl.BlockSpec((rows, WIDE), lambda j: (0, j))],
        pl.BlockSpec((ROWS, WIDE, WIDE), lambda j: (0, j, 0)),
        (x,),
        grid=(CHUNKS,),
        name="cells_first",
    )


def pick_rows(which, wanted_ref, table_ref, out_ref):
    def per_across(z, _):
        def some(i, _):
            for u in range(32):
                s = i * 32 + u
                out_ref[pl.ds(z * SLOTS + s, 1), :] = table_ref[pl.ds(wanted_ref[z * 1024 + which * 384 + s], 1), :]
            return 0

        return lax.fori_loop(0, SLOTS // 32, some, 0)

    lax.fori_loop(0, 4, per_across, 0)


def pick_body(which, wanted_ref, table_ref, out_ref):
    pick_rows(which, wanted_ref, table_ref, out_ref)


def pick_back_body(which, along_ref, w1, w2, w3, table_ref, o1, o2, o3):
    @pl.when(along_ref[0] < SPAN)
    def _():
        for w, o in ((w1, o1), (w2, o2), (w3, o3)):
            pick_rows(which, w, table_ref, o)


MESSAGE = jax.ShapeDtypeStruct((4 * SLOTS, WIDE), F32)


def pick(which, wanted, table):
    return kernel_call(
        functools.partial(pick_body, which), MESSAGE, [SMEM, VMEM], VMEM, (wanted, table), flops=1 << 24, name="pick"
    )


def pick_back(which, along, wanted, table):
    return kernel_call(
        functools.partial(pick_back_body, which),
        (MESSAGE,) * 3,
        [SMEM] * 4 + [VMEM],
        (VMEM,) * 3,
        (along, *wanted, table),
        name="pick_back",
    )


def place_body(which, own_ref, x0, x1, x2, x3, weight_ref, out_ref, cells):
    for kind, x in enumerate((x0, x1, x2, x3)):
        def per_across(z, _, kind=kind, x=x):
            def some(i, _):
                for u in range(32):
                    s = i * 32 + u
                    cell = own_ref[(z * SPAN + kind) * 1024 + which * 384 + s]
                    cells[pl.ds(cell, 1), :] = x[pl.ds(z * SLOTS + s, 1), :]
                return 0

            return lax.fori_loop(0, SLOTS // 32, some, 0)

        lax.fori_loop(0, 4, per_across, 0)
    lane = iota((64, WIDE), 1)
    top = (lane == LAYERS - 1) | (lane == 2 * LAYERS - 1) | (lane == 3 * LAYERS - 1)

    def mix(i, _):
        rows = pl.ds(pl.multiple_of(i * 64, 64), 64)
        here = cells[rows, :]
        upper = jnp.where(top, here, pltpu.roll(here, WIDE - 1, 1))
        weight = weight_ref[rows, :]
        out_ref[rows, :] = (1.0 - weight) * here + weight * upper
        return 0

    lax.fori_loop(0, CELLS // 64, mix, 0)


def place(which, own, xs, weight):
    return kernel_call(
        functools.partial(place_body, which),
        jax.ShapeDtypeStruct((CELLS, WIDE), F32),
        [SMEM] + [VMEM] * 5,
        VMEM,
        (own, *xs, weight),
        scratch=[pltpu.VMEM((CELLS + 8, WIDE), F32)],
        name="place",
    )


def pivots_body(mix_ref, drag_ref, out_ref):
    for which in range(2):
        factor = None
        for k in range(LAYERS):
            below = None if k == 0 else mix_ref[(which * 39 + k - 1) * 8 : (which * 39 + k) * 8, :]
            above = None if k == LAYERS - 1 else mix_ref[(which * 39 + k) * 8 : (which * 39 + k + 1) * 8, :]
            diagonal = 1.0
            for term in (below, above):
                if term is not None:
                    diagonal = diagonal + term
            if k == 0 and which == 0:
                diagonal = diagonal + drag_ref[...]
            if k > 0:
                diagonal = diagonal - below * factor
            inverse = 1.0 / diagonal
            out_ref[(which * LAYERS + k) * 8 : (which * LAYERS + k + 1) * 8, :] = inverse
            if above is not None:
                factor = above * inverse


def pivots(mix, drag):
    return kernel_call(
        pivots_body,
        jax.ShapeDtypeStruct((2 * LAYERS * 8, COLS), F32),
        [pl.BlockSpec((2 * 39 * 8, WIDE), lambda j: (0, j)), pl.BlockSpec((8, WIDE), lambda j: (0, j))],
        pl.BlockSpec((2 * LAYERS * 8, WIDE), lambda j: (0, j)),
        (mix, drag),
        grid=(CHUNKS,),
        name="pivots",
    )


def layers_body(x_ref, o_ref):
    for row in range(ROWS):
        o_ref[pl.ds(row, LEVELS, stride=8), :] = x_ref[row].T[0:LEVELS, :]


def layers_first(x):
    return kernel_call(
        layers_body,
        jax.ShapeDtypeStruct((CHUNKS * LEVELS * 8, WIDE), F32),
        [pl.BlockSpec((ROWS, WIDE, WIDE), lambda j: (0, j, 0))],
        pl.BlockSpec((LEVELS * 8, WIDE), lambda j: (j, 0)),
        (x,),
        grid=(CHUNKS,),
        name="layers_first",
    )


def solve_body(
    place_ref, moved_ref, up_ref, down_ref, left_ref, right_ref, lateral_ref, mix_ref, inverse_ref, stress_ref, out_ref, edge
):
    j = pl.program_id(0)
    sub, lane = iota((8, WIDE), 0), iota((8, WIDE), 1)
    size = LEVELS * 8

    def spread(source_ref):
        source = source_ref[...]
        for level in range(LEVELS):
            edge[level * 8 : level * 8 + 8, :] = jnp.broadcast_to(source[:, level : level + 1], (8, WIDE))

    @pl.when(j == 0)
    def _():
        spread(left_ref)

    @pl.when(j == CHUNKS - 1)
    def _():
        spread(right_ref)

    start = pl.multiple_of(j * size, size)
    before = pl.multiple_of(jnp.maximum(j - 1, 0) * size, size)
    after = pl.multiple_of(jnp.minimum(j + 1, CHUNKS - 1) * size, size)
    up, down = up_ref[...].T, down_ref[...].T
    lateral = lateral_ref[...]
    count = 4.0 - (
        ((place_ref[0] == 0) & (j == 0) & (lane == 0)).astype(F32)
        + ((place_ref[0] == 31) & (j == CHUNKS - 1) & (lane == WIDE - 1)).astype(F32)
        + ((place_ref[1] == 0) & (sub == 0)).astype(F32)
        + ((place_ref[1] == 3) & (sub == 7)).astype(F32)
    )
    first_chunk, last_chunk = j == 0, j == CHUNKS - 1
    for m in range(3):
        which = 0 if m < 2 else 1
        value = None
        for k in range(LAYERS):
            level = m * LAYERS + k
            at = level * 8
            here = moved_ref[pl.ds(start + at, 8), :]
            halo = edge[at : at + 8, :]
            lower = jnp.where(first_chunk, halo, moved_ref[pl.ds(before + at, 8), :])
            upper = jnp.where(last_chunk, halo, moved_ref[pl.ds(after + at, 8), :])
            west = jnp.where(lane == 0, pltpu.roll(lower, 1, 1), pltpu.roll(here, 1, 1))
            east = jnp.where(lane == WIDE - 1, pltpu.roll(upper, WIDE - 1, 1), pltpu.roll(here, WIDE - 1, 1))
            north = jnp.where(sub == 0, up[level : level + 1, :], pltpu.roll(here, 1, 0))
            south = jnp.where(sub == 7, down[level : level + 1, :], pltpu.roll(here, 7, 0))
            source = here + lateral * (((north + south) + west) + east - count * here)
            if k == LAYERS - 1 and m < 2:
                source = source + stress_ref[m * 8 : m * 8 + 8, :]
            if k > 0:
                source = source + mix_ref[(which * 39 + k - 1) * 8 : (which * 39 + k) * 8, :] * value
            value = source * inverse_ref[(which * LAYERS + k) * 8 : (which * LAYERS + k + 1) * 8, :]
            out_ref[(k * 3 + m) * 8 : (k * 3 + m + 1) * 8, :] = value
        for k in range(LAYERS - 2, -1, -1):
            rows = slice((k * 3 + m) * 8, (k * 3 + m + 1) * 8)
            factor = (
                mix_ref[(which * 39 + k) * 8 : (which * 39 + k + 1) * 8, :]
                * inverse_ref[(which * LAYERS + k) * 8 : (which * LAYERS + k + 1) * 8, :]
            )
            value = out_ref[rows, :] + factor * value
            out_ref[rows, :] = value


def solve(where, moved, up, down, left, right, lateral, mix, inverse, stress):
    def chunk(rows):
        return pl.BlockSpec((rows, WIDE), lambda j: (0, j))

    def cells(rows):
        return pl.BlockSpec((rows, WIDE), lambda j: (j, 0))

    def fixed(rows):
        return pl.BlockSpec((rows, WIDE), lambda j: (0, 0))

    return kernel_call(
        solve_body,
        jax.ShapeDtypeStruct((LEVELS * 8, COLS), F32),
        [
            SMEM,
            fixed(CHUNKS * LEVELS * 8),
            cells(WIDE),
            cells(WIDE),
            fixed(8),
            fixed(8),
            chunk(8),
            chunk(2 * 39 * 8),
            chunk(2 * LAYERS * 8),
            chunk(16),
        ],
        chunk(LEVELS * 8),
        (where, moved, up, down, left, right, lateral, mix, inverse, stress),
        grid=(CHUNKS,),
        scratch=[pltpu.VMEM((LEVELS * 8, WIDE), F32)],
        name="solve",
    )


def move(x, axis, distance, low=0, high=None):
    count = lax.axis_size(axis)
    high = count if high is None else high
    pairs = [(i, i + distance) for i in range(low, high) if 0 <= i + distance < count]
    return lax.ppermute(x, axis, pairs)


def body(fields, first_feet, first_fraction, second_feet, second_fraction, lateral_mix, vertical_mix, bottom_drag, surface_stress):
    along = lax.axis_index("along")
    across = lax.axis_index("across")
    where = jnp.stack([along, across]).astype(I32)

    wanted, own = kernel_call(
        slots_body,
        (jax.ShapeDtypeStruct((128, WIDE), I32),) * 2,
        [SMEM, VMEM, VMEM],
        (VMEM, VMEM),
        (where, first_feet, second_feet),
        name="slots",
    )
    own = own.reshape(-1)
    wanted = lax.all_to_all(wanted.reshape(4, SPAN, 8, WIDE), "across", split_axis=0, concat_axis=0, tiled=True)
    ahead = [wanted[:, 0]] + [move(wanted[:, t], "along", -t) for t in range(1, SPAN)]
    back = []
    for u in range(1, SPAN):
        payload = lax.dynamic_index_in_dim(wanted, jnp.minimum(along + u, SPAN - 1), axis=1, keepdims=False)
        pairs = [(i, i + u) for i in range(SPAN - u)]
        back.append(lax.ppermute(payload, "along", pairs))
    ahead = [x.reshape(-1) for x in ahead]
    back = [x.reshape(-1) for x in back]

    def fetch(which, table):
        sent = {}
        for t in (3, 2, 1):
            sent[t] = move(pick(which, ahead[t], table), "along", t)
        behind = [
            lax.ppermute(x, "along", [(i, i - u) for i in range(u, SPAN)])
            for u, x in zip((1, 2, 3), pick_back(which, where, back, table))
        ]
        parts = [pick(which, ahead[0], table)]
        for t in range(1, SPAN):
            part = sent[t]
            for a in range(t):
                part = jnp.where(along == a, behind[t - a - 1], part)
            parts.append(part)
        return [
            lax.all_to_all(x.reshape(4, SLOTS, WIDE), "across", split_axis=0, concat_axis=0, tiled=True).reshape(-1, WIDE)
            for x in parts
        ]

    table = cells_first(fields.reshape(LEVELS * 8, COLS), 1).reshape(CELLS, WIDE)
    first_weight = cells_first(first_fraction.reshape(LAYERS * 8, COLS), 3).reshape(CELLS, WIDE)
    second_weight = cells_first(second_fraction.reshape(LAYERS * 8, COLS), 3).reshape(CELLS, WIDE)
    mix = vertical_mix.reshape(2 * 39 * 8, COLS)
    inverse = pivots(mix, bottom_drag)

    middle = place(0, own, fetch(0, table), first_weight)
    moved = place(1, own, fetch(1, middle), second_weight).reshape(ROWS, COLS, WIDE)
    up = move(moved[ROWS - 1], "across", 1)
    down = move(moved[0], "across", -1)
    left = move(moved[:, COLS - 1], "along", 1)
    right = move(moved[:, 0], "along", -1)
    result = solve(
        where, layers_first(moved), up, down, left, right, lateral_mix, mix, inverse, surface_stress.reshape(16, COLS)
    )
    return result.reshape(LAYERS, 3, ROWS, COLS)


def solution(mesh):
    in_specs = (
        P(None, None, "across", "along"),
        P("across", "along"),
        P(None, "across", "along"),
        P("across", "along"),
        P(None, "across", "along"),
        P("across", "along"),
        P(None, None, "across", "along"),
        P("across", "along"),
        P(None, "across", "along"),
    )
    out_specs = P(None, None, "across", "along")
    return jax.shard_map(body, mesh=mesh, in_specs=in_specs, out_specs=out_specs, check_vma=False)
```

```python
import functools

import jax
import jax.numpy as jnp
from jax import lax
from jax.experimental import pallas as pl
from jax.experimental.pallas import tpu as pltpu
from jax.sharding import PartitionSpec as P


LAYERS = 40
ROWS = 8
COLS = 512
CELLS = ROWS * COLS
SLOTS = 288
SPAN = 4
ORDER = (1, 2, 3)
WIDE = 128
CHUNKS = COLS // WIDE
LEVELS = 3 * LAYERS
F32 = jnp.float32
I32 = jnp.int32
VMEM = pl.BlockSpec(memory_space=pltpu.VMEM)
SMEM = pl.BlockSpec(memory_space=pltpu.SMEM)
ANY = pl.BlockSpec(memory_space=pl.ANY)


def iota(shape, dim):
    return lax.broadcasted_iota(I32, shape, dim)


def kernel_call(body, out_shapes, in_specs, out_specs, operands, flops=1 << 20, grid=None, scratch=(), limit=6):
    extra = {} if grid is None else {"grid": grid}
    return pl.pallas_call(
        body,
        out_shape=out_shapes,
        in_specs=in_specs,
        out_specs=out_specs,
        scratch_shapes=list(scratch),
        cost_estimate=pl.CostEstimate(flops=flops, bytes_accessed=1 << 21, transcendentals=0),
        compiler_params=pltpu.CompilerParams(vmem_limit_bytes=limit << 20),
        **extra,
    )(*operands)


def slots_body(along_ref, first_ref, second_ref, wanted_ref, own_ref):
    along = along_ref[0]
    before = (iota((COLS, COLS), 0) < iota((COLS, COLS), 1)).astype(F32).astype(jnp.bfloat16)
    partner_rows = iota((16, COLS), 0)
    slot_rows = iota((48, COLS), 0)
    lane_rows = iota((WIDE, COLS), 0)
    lane = iota((1, COLS), 1)
    wanted_ref[...] = jnp.zeros((128, WIDE), I32)
    for which, feet_ref in enumerate((first_ref, second_ref)):
        carry = jnp.zeros((16, 1), F32)
        total = jnp.zeros((192, WIDE), F32)
        for row in range(ROWS):
            feet = feet_ref[row : row + 1, :]
            global_row = feet >> 14
            column = feet & 16383
            across = global_row >> 3
            owner = column >> 9
            local = (global_row & 7) * COLS + (column & 511)
            kind = jnp.where(owner <= along, along - owner, owner)
            partner = across * SPAN + kind
            mask = partner_rows == partner
            ones = mask.astype(F32)
            prefix = jnp.dot(ones.astype(jnp.bfloat16), before, preferred_element_type=F32)
            rank = jnp.sum(jnp.where(mask, prefix + carry, 0.0), axis=0, keepdims=True).astype(I32)
            carry = carry + jnp.sum(ones, axis=1, keepdims=True)
            hit = slot_rows == partner * 3 + (rank >> 7)
            spot = (lane_rows == (rank & 127)).astype(F32).astype(jnp.bfloat16)
            own = CELLS - (row * COLS + lane)
            values = []
            for value in (local & 63, local >> 6, own & 63, own >> 6):
                values.append(jnp.where(hit, value.astype(F32), 0.0).astype(jnp.bfloat16))
            total = total + lax.dot_general(
                jnp.concatenate(values, axis=0),
                spot,
                (((1,), (1,)), ((), ())),
                preferred_element_type=F32,
            )
        whole = total.astype(I32)
        wanted = whole[0:48] + whole[48:96] * 64
        own = CELLS - (whole[96:144] + whole[144:192] * 64)
        for z in range(4):
            for kind in range(SPAN):
                partner = z * SPAN + kind
                wanted_ref[partner * 8 + which * 3 : partner * 8 + which * 3 + 3, :] = wanted[partner * 3 : partner * 3 + 3]
                place = (which * SPAN + kind) * 16 + z * 4
                own_ref[place : place + 3, :] = own[partner * 3 : partner * 3 + 3]


def table_body(copies, x_ref, *refs):
    o_ref = refs[-1]
    for row in range(ROWS):
        if copies == 1:
            parts = [x_ref[pl.ds(m * 8 + row, LAYERS, stride=24), :] for m in range(3)]
        else:
            part = x_ref[pl.ds(row, LAYERS, stride=8), :]
            part = jnp.where(iota((LAYERS, WIDE), 0) == LAYERS - 1, 0.0, part)
            parts = [part, part, part]
        parts.append(jnp.zeros((WIDE - LEVELS, WIDE), F32))
        o_ref[row] = jnp.concatenate(parts, axis=0).T


def cells_first(x, copies, *after):
    rows = x.shape[0]
    return kernel_call(
        functools.partial(table_body, copies),
        jax.ShapeDtypeStruct((ROWS, COLS, WIDE), F32),
        [pl.BlockSpec((rows, WIDE), lambda j: (0, j))] + [ANY] * len(after),
        pl.BlockSpec((ROWS, WIDE, WIDE), lambda j: (0, j, 0)),
        (x, *after),
        grid=(CHUNKS,),
    )


def copy_rows(source, target, from_row, to_row, index_of):
    def some(i, _):
        for u in range(32):
            s = i * 32 + u
            index = index_of(s)
            target[pl.ds(to_row(s, index), 1), :] = source[pl.ds(from_row(s, index), 1), :]
        return 0

    lax.fori_loop(0, SLOTS // 32, some, 0)


def pick_rows(which, wanted_ref, table_ref, out_ref, pitch=SLOTS):
    def per_across(z, _):
        copy_rows(
            table_ref,
            out_ref,
            lambda s, index: index,
            lambda s, index: z * pitch + s,
            lambda s: wanted_ref[z * 1024 + which * 384 + s],
        )
        return 0

    lax.fori_loop(0, 4, per_across, 0)


def pick_body(which, wanted_ref, table_ref, *refs):
    pick_rows(which, wanted_ref, table_ref, refs[-1])


MESSAGE = jax.ShapeDtypeStruct((4 * SLOTS, WIDE), F32)


def pick(which, wanted, table, *after):
    return kernel_call(
        functools.partial(pick_body, which),
        MESSAGE,
        [SMEM, VMEM] + [ANY] * len(after),
        VMEM,
        (wanted, table, *after),
        flops=1 << 28,
    )


def pick_back_body(which, along_ref, w1, w2, w3, table, after, o1, o2, o3, wanted, sem):
    for u, w, o in ((1, w1, o1), (2, w2, o2), (3, w3, o3)):

        @pl.when((along_ref[0] < SPAN) & (along_ref[0] >= u))
        def _(w=w, o=o):
            load = pltpu.make_async_copy(w, wanted, sem)
            load.start()
            load.wait()
            pick_rows(which, wanted, table, o)


def pick_back(which, along, wanted, table, after):
    return kernel_call(
        functools.partial(pick_back_body, which),
        (MESSAGE,) * 3,
        [SMEM] + [ANY] * 3 + [VMEM, ANY],
        (VMEM,) * 3,
        (along, *wanted, table, after),
        scratch=[pltpu.SMEM((4096,), I32), pltpu.SemaphoreType.DMA],
    )


def put_class(along_ref, kind, spot, x_ref, backs, out_ref, buffer, sem):
    def put(source):
        for z in range(4):
            start = (2 * z + spot) * SLOTS
            out_ref[start : start + SLOTS, :] = source[z * SLOTS : (z + 1) * SLOTS, :]

    put(x_ref)
    for a in range(kind):

        @pl.when(along_ref[0] == a)
        def _(a=a):
            load = pltpu.make_async_copy(backs[kind - a - 1], buffer, sem)
            load.start()
            load.wait()
            put(buffer)


PAIR = jax.ShapeDtypeStruct((8 * SLOTS, WIDE), F32)


def pick_join_body(which, kind, along_ref, wanted_ref, table_ref, x_ref, *refs):
    out_ref, buffer, sem = refs[-3:]
    pick_rows(which, wanted_ref, table_ref, out_ref, 2 * SLOTS)
    put_class(along_ref, kind, 1, x_ref, refs[:kind], out_ref, buffer, sem)


def pick_join(which, kind, along, wanted, table, x, backs, *after):
    return kernel_call(
        functools.partial(pick_join_body, which, kind),
        PAIR,
        [SMEM, SMEM, VMEM, VMEM] + [ANY] * (kind + len(after)),
        VMEM,
        (along, wanted, table, x, *backs[:kind], *after),
        scratch=[pltpu.VMEM((4 * SLOTS, WIDE), F32), pltpu.SemaphoreType.DMA],
        flops=1 << 28,
        limit=8,
    )


def join_body(kinds, along_ref, x_ref, y_ref, b1, b2, b3, *refs):
    out_ref, buffer, sem = refs[-3:]
    for spot, (kind, ref) in enumerate(zip(kinds, (x_ref, y_ref))):
        put_class(along_ref, kind, spot, ref, (b1, b2, b3), out_ref, buffer, sem)


def join(kinds, along, x, y, backs, *after):
    return kernel_call(
        functools.partial(join_body, kinds),
        PAIR,
        [SMEM, VMEM, VMEM] + [ANY] * (3 + len(after)),
        VMEM,
        (along, x, y, *backs, *after),
        scratch=[pltpu.VMEM((4 * SLOTS, WIDE), F32), pltpu.SemaphoreType.DMA],
        flops=1 << 27,
        limit=8,
    )


def put_rows(own_ref, x, cells, pitch=SLOTS, start=0):
    def per_across(z, _):
        copy_rows(
            x,
            cells,
            lambda s, index: z * pitch + start + s,
            lambda s, index: index,
            lambda s: own_ref[z * 512 + s],
        )
        return 0

    lax.fori_loop(0, 4, per_across, 0)


def load_own(which, kinds, own_any, own, sems):
    loads = [
        pltpu.make_async_copy(own_any.at[pl.ds((which * SPAN + kind) * 2048, 2048)], own[i], sems.at[i])
        for i, kind in enumerate(kinds)
    ]
    for load in loads:
        load.start()
    return loads


def place_early_body(which, kinds, own_any, x, after, cells, own0, own1, sems):
    for i, load in enumerate(load_own(which, kinds, own_any, (own0, own1), sems)):
        load.wait()
        put_rows((own0, own1)[i], x, cells, 2 * SLOTS, i * SLOTS)


def place_early(which, kinds, own, x, after):
    return kernel_call(
        functools.partial(place_early_body, which, kinds),
        jax.ShapeDtypeStruct((CELLS + 8, WIDE), F32),
        [ANY, VMEM, ANY],
        VMEM,
        (own, x, after),
        scratch=[*([pltpu.SMEM((2048,), I32)] * 2), pltpu.SemaphoreType.DMA((2,))],
        flops=1 << 28,
    )


def place_body(which, kinds, own_any, cells_ref, x, weight_ref, out_ref, cells, own0, own1, sems):
    loads = load_own(which, kinds, own_any, (own0, own1), sems)
    cells[...] = cells_ref[...]
    for i, load in enumerate(loads):
        load.wait()
        put_rows((own0, own1)[i], x, cells, 2 * SLOTS, i * SLOTS)

    def mix(i, _):
        rows = pl.ds(pl.multiple_of(i * 128, 128), 128)
        here = cells[rows, :]
        upper = pltpu.roll(here, WIDE - 1, 1)
        out_ref[rows, :] = here + weight_ref[rows, :] * (upper - here)
        return 0

    lax.fori_loop(0, CELLS // 128, mix, 0)


def place(which, kinds, own, cells, x, weight):
    return kernel_call(
        functools.partial(place_body, which, kinds),
        jax.ShapeDtypeStruct((CELLS, WIDE), F32),
        [ANY] + [VMEM] * 3,
        VMEM,
        (own, cells, x, weight),
        scratch=[
            pltpu.VMEM((CELLS + 8, WIDE), F32),
            *([pltpu.SMEM((2048,), I32)] * 2),
            pltpu.SemaphoreType.DMA((2,)),
        ],
        flops=1 << 28,
        limit=12,
    )


def pivots_body(mix_ref, drag_ref, after_ref, out_ref):
    for which in range(2):
        factor = None
        for k in range(LAYERS):
            below = None if k == 0 else mix_ref[(which * 39 + k - 1) * 8 : (which * 39 + k) * 8, :]
            above = None if k == LAYERS - 1 else mix_ref[(which * 39 + k) * 8 : (which * 39 + k + 1) * 8, :]
            diagonal = 1.0
            for term in (below, above):
                if term is not None:
                    diagonal = diagonal + term
            if k == 0 and which == 0:
                diagonal = diagonal + drag_ref[...]
            if k > 0:
                diagonal = diagonal - below * factor
            inverse = 1.0 / diagonal
            out_ref[(which * LAYERS + k) * 8 : (which * LAYERS + k + 1) * 8, :] = inverse
            if above is not None:
                factor = above * inverse


def pivots(mix, drag, after):
    return kernel_call(
        pivots_body,
        jax.ShapeDtypeStruct((2 * LAYERS * 8, COLS), F32),
        [pl.BlockSpec((2 * 39 * 8, WIDE), lambda j: (0, j)), pl.BlockSpec((8, WIDE), lambda j: (0, j)), ANY],
        pl.BlockSpec((2 * LAYERS * 8, WIDE), lambda j: (0, j)),
        (mix, drag, after),
        grid=(CHUNKS,),
    )


def layers_body(x_ref, o_ref):
    for row in range(ROWS):
        o_ref[pl.ds(row, LEVELS, stride=8), :] = x_ref[row].T[0:LEVELS, :]


def layers_first(x):
    return kernel_call(
        layers_body,
        jax.ShapeDtypeStruct((CHUNKS * LEVELS * 8, WIDE), F32),
        [pl.BlockSpec((ROWS, WIDE, WIDE), lambda j: (0, j, 0))],
        pl.BlockSpec((LEVELS * 8, WIDE), lambda j: (j, 0)),
        (x,),
        grid=(CHUNKS,),
    )


def solve_body(
    place_ref, moved_ref, up_ref, down_ref, left_ref, right_ref, lateral_ref, mix_ref, inverse_ref, stress_ref, out_ref, edge
):
    j = pl.program_id(0)
    sub, lane = iota((8, WIDE), 0), iota((8, WIDE), 1)
    size = LEVELS * 8

    def spread(source_ref):
        source = source_ref[...]
        for level in range(LEVELS):
            edge[level * 8 : level * 8 + 8, :] = jnp.broadcast_to(source[:, level : level + 1], (8, WIDE))

    @pl.when(j == 0)
    def _():
        spread(left_ref)

    @pl.when(j == CHUNKS - 1)
    def _():
        spread(right_ref)

    start = pl.multiple_of(j * size, size)
    before = pl.multiple_of(jnp.maximum(j - 1, 0) * size, size)
    after = pl.multiple_of(jnp.minimum(j + 1, CHUNKS - 1) * size, size)
    up, down = up_ref[...].T, down_ref[...].T
    lateral = lateral_ref[...]
    count = 4.0 - (
        ((place_ref[0] == 0) & (j == 0) & (lane == 0)).astype(F32)
        + ((place_ref[0] == 31) & (j == CHUNKS - 1) & (lane == WIDE - 1)).astype(F32)
        + ((place_ref[1] == 0) & (sub == 0)).astype(F32)
        + ((place_ref[1] == 3) & (sub == 7)).astype(F32)
    )
    first_chunk, last_chunk = j == 0, j == CHUNKS - 1
    for m in range(3):
        which = 0 if m < 2 else 1
        value = None
        for k in range(LAYERS):
            level = m * LAYERS + k
            at = level * 8
            here = moved_ref[pl.ds(start + at, 8), :]
            halo = edge[at : at + 8, :]
            lower = jnp.where(first_chunk, halo, moved_ref[pl.ds(before + at, 8), :])
            upper = jnp.where(last_chunk, halo, moved_ref[pl.ds(after + at, 8), :])
            west = jnp.where(lane == 0, pltpu.roll(lower, 1, 1), pltpu.roll(here, 1, 1))
            east = jnp.where(lane == WIDE - 1, pltpu.roll(upper, WIDE - 1, 1), pltpu.roll(here, WIDE - 1, 1))
            north = jnp.where(sub == 0, up[level : level + 1, :], pltpu.roll(here, 1, 0))
            south = jnp.where(sub == 7, down[level : level + 1, :], pltpu.roll(here, 7, 0))
            source = here + lateral * (((north + south) + west) + east - count * here)
            if k == LAYERS - 1 and m < 2:
                source = source + stress_ref[m * 8 : m * 8 + 8, :]
            if k > 0:
                source = source + mix_ref[(which * 39 + k - 1) * 8 : (which * 39 + k) * 8, :] * value
            value = source * inverse_ref[(which * LAYERS + k) * 8 : (which * LAYERS + k + 1) * 8, :]
            out_ref[(k * 3 + m) * 8 : (k * 3 + m + 1) * 8, :] = value
        for k in range(LAYERS - 2, -1, -1):
            rows = slice((k * 3 + m) * 8, (k * 3 + m + 1) * 8)
            factor = (
                mix_ref[(which * 39 + k) * 8 : (which * 39 + k + 1) * 8, :]
                * inverse_ref[(which * LAYERS + k) * 8 : (which * LAYERS + k + 1) * 8, :]
            )
            value = out_ref[rows, :] + factor * value
            out_ref[rows, :] = value


def solve(where, moved, up, down, left, right, lateral, mix, inverse, stress):
    def chunk(rows):
        return pl.BlockSpec((rows, WIDE), lambda j: (0, j))

    def cells(rows):
        return pl.BlockSpec((rows, WIDE), lambda j: (j, 0))

    def fixed(rows):
        return pl.BlockSpec((rows, WIDE), lambda j: (0, 0))

    return kernel_call(
        solve_body,
        jax.ShapeDtypeStruct((LEVELS * 8, COLS), F32),
        [
            SMEM,
            fixed(CHUNKS * LEVELS * 8),
            cells(WIDE),
            cells(WIDE),
            fixed(8),
            fixed(8),
            chunk(8),
            chunk(2 * 39 * 8),
            chunk(2 * LAYERS * 8),
            chunk(16),
        ],
        chunk(LEVELS * 8),
        (where, moved, up, down, left, right, lateral, mix, inverse, stress),
        grid=(CHUNKS,),
        scratch=[pltpu.VMEM((LEVELS * 8, WIDE), F32)],
        limit=14,
    )


def move(x, axis, distance, low=0, high=None):
    count = lax.axis_size(axis)
    high = count if high is None else high
    pairs = [(i, i + distance) for i in range(low, high) if 0 <= i + distance < count]
    return lax.ppermute(x, axis, pairs)


def body(fields, first_feet, first_fraction, second_feet, second_fraction, lateral_mix, vertical_mix, bottom_drag, surface_stress):
    along = lax.axis_index("along")
    across = lax.axis_index("across")
    where = jnp.stack([along, across]).astype(I32)

    wanted, own = kernel_call(
        slots_body,
        (jax.ShapeDtypeStruct((128, WIDE), I32),) * 2,
        [SMEM, VMEM, VMEM],
        (VMEM,) * 2,
        (where, first_feet, second_feet),
    )
    wanted = lax.all_to_all(wanted.reshape(4, SPAN, 8, WIDE), "across", split_axis=0, concat_axis=0, tiled=True)
    ahead = [wanted[:, 0]] + [move(wanted[:, t], "along", -t) for t in range(1, SPAN)]
    back = []
    for u in range(1, SPAN):
        payload = lax.dynamic_index_in_dim(wanted, jnp.minimum(along + u, SPAN - 1), axis=1, keepdims=False)
        pairs = [(i, i + u) for i in range(SPAN - u)]
        back.append(lax.ppermute(payload, "along", pairs))
    own = own.reshape(-1)
    ahead = [x.reshape(-1) for x in ahead]
    back = [x.reshape(-1) for x in back]

    def turn(x):
        x = x.reshape(4, 2 * SLOTS, WIDE)
        return lax.all_to_all(x, "across", split_axis=0, concat_axis=0, tiled=True).reshape(-1, WIDE)

    def fetch(which, table, weigh):
        i, j, k = ORDER
        pi = pick(which, ahead[i], table, *ahead[1:], *back)
        pj = pick(which, ahead[j], table, pi)
        pk = pick(which, ahead[k], table, pj)
        xi, xj, xk = [move(p, "along", t) for t, p in ((i, pi), (j, pj), (k, pk))]
        behind = [
            lax.ppermute(x, "along", [(b, b - u) for b in range(u, SPAN)])
            for u, x in zip((1, 2, 3), pick_back(which, where, back, table, pk))
        ]
        weight, done = weigh(pk)
        joined = pick_join(which, i, where, ahead[0], table, xi, behind, pk, *done)
        early = turn(joined)
        cells = place_early(which, (0, i), own, early, joined)
        late = turn(join((j, k), where, xj, xk, behind, cells))
        return place(which, (j, k), own, cells, late, weight)

    mix = vertical_mix.reshape(2 * 39 * 8, COLS)
    inverse = []

    def first_weight(after):
        inverse.append(pivots(mix, bottom_drag, after))
        weight = cells_first(first_fraction.reshape(LAYERS * 8, COLS), 3, after)
        return weight.reshape(CELLS, WIDE), (weight, inverse[0])

    def second_weight(after):
        weight = cells_first(second_fraction.reshape(LAYERS * 8, COLS), 3, after)
        return weight.reshape(CELLS, WIDE), (weight,)

    table = cells_first(fields.reshape(LEVELS * 8, COLS), 1).reshape(CELLS, WIDE)
    middle = fetch(0, table, first_weight)
    moved = fetch(1, middle, second_weight).reshape(ROWS, COLS, WIDE)
    up = move(moved[ROWS - 1], "across", 1)
    down = move(moved[0], "across", -1)
    left = move(moved[:, COLS - 1], "along", 1)
    right = move(moved[:, 0], "along", -1)
    result = solve(
        where, layers_first(moved), up, down, left, right, lateral_mix, mix, inverse[0], surface_stress.reshape(16, COLS)
    )
    return result.reshape(LAYERS, 3, ROWS, COLS)


def solution(mesh):
    in_specs = (
        P(None, None, "across", "along"),
        P("across", "along"),
        P(None, "across", "along"),
        P("across", "along"),
        P(None, "across", "along"),
        P("across", "along"),
        P(None, None, "across", "along"),
        P("across", "along"),
        P(None, "across", "along"),
    )
    out_specs = P(None, None, "across", "along")
    return jax.shard_map(body, mesh=mesh, in_specs=in_specs, out_specs=out_specs, check_vma=False)
```

```python
import functools

import jax
import jax.numpy as jnp
from jax import lax
from jax.experimental import pallas as pl
from jax.experimental.pallas import tpu as pltpu
from jax.sharding import PartitionSpec as P


LAYERS = 40
ROWS = 8
COLS = 512
CELLS = ROWS * COLS
SLOTS = 288
SPAN = 4
WIDE = 128
CHUNKS = COLS // WIDE
LEVELS = 3 * LAYERS
F32 = jnp.float32
I32 = jnp.int32
VMEM = pl.BlockSpec(memory_space=pltpu.VMEM)
SMEM = pl.BlockSpec(memory_space=pltpu.SMEM)
ANY = pl.BlockSpec(memory_space=pl.ANY)


def iota(shape, dim):
    return lax.broadcasted_iota(I32, shape, dim)


def kernel_call(body, out_shapes, in_specs, out_specs, operands, flops=1 << 20, grid=None, scratch=(), limit=6):
    extra = {} if grid is None else {"grid": grid}
    return pl.pallas_call(
        body,
        out_shape=out_shapes,
        in_specs=in_specs,
        out_specs=out_specs,
        scratch_shapes=list(scratch),
        cost_estimate=pl.CostEstimate(flops=flops, bytes_accessed=1 << 21, transcendentals=0),
        compiler_params=pltpu.CompilerParams(vmem_limit_bytes=limit << 20),
        **extra,
    )(*operands)


def slots_body(along_ref, first_ref, second_ref, wanted_ref, own_ref):
    along = along_ref[0]
    before = (iota((COLS, COLS), 0) < iota((COLS, COLS), 1)).astype(F32).astype(jnp.bfloat16)
    partner_rows = iota((16, COLS), 0)
    slot_rows = iota((48, COLS), 0)
    lane_rows = iota((WIDE, COLS), 0)
    lane = iota((1, COLS), 1)
    wanted_ref[...] = jnp.zeros((128, WIDE), I32)
    for which, feet_ref in enumerate((first_ref, second_ref)):
        carry = jnp.zeros((16, 1), F32)
        total = jnp.zeros((192, WIDE), F32)
        for row in range(ROWS):
            feet = feet_ref[row : row + 1, :]
            global_row = feet >> 14
            column = feet & 16383
            across = global_row >> 3
            owner = column >> 9
            local = (global_row & 7) * COLS + (column & 511)
            kind = jnp.where(owner <= along, along - owner, owner)
            partner = across * SPAN + kind
            mask = partner_rows == partner
            ones = mask.astype(F32)
            prefix = jnp.dot(ones.astype(jnp.bfloat16), before, preferred_element_type=F32)
            rank = jnp.sum(jnp.where(mask, prefix + carry, 0.0), axis=0, keepdims=True).astype(I32)
            carry = carry + jnp.sum(ones, axis=1, keepdims=True)
            hit = slot_rows == partner * 3 + (rank >> 7)
            spot = (lane_rows == (rank & 127)).astype(F32).astype(jnp.bfloat16)
            own = CELLS - (row * COLS + lane)
            values = []
            for value in (local & 63, local >> 6, own & 63, own >> 6):
                values.append(jnp.where(hit, value.astype(F32), 0.0).astype(jnp.bfloat16))
            total = total + lax.dot_general(
                jnp.concatenate(values, axis=0),
                spot,
                (((1,), (1,)), ((), ())),
                preferred_element_type=F32,
            )
        whole = total.astype(I32)
        wanted = whole[0:48] + whole[48:96] * 64
        own = CELLS - (whole[96:144] + whole[144:192] * 64)
        for z in range(4):
            for kind in range(SPAN):
                partner = z * SPAN + kind
                wanted_ref[partner * 8 + which * 3 : partner * 8 + which * 3 + 3, :] = wanted[partner * 3 : partner * 3 + 3]
                place = (which * SPAN + kind) * 16 + z * 4
                own_ref[place : place + 3, :] = own[partner * 3 : partner * 3 + 3]


def table_body(copies, x_ref, *refs):
    o_ref = refs[-1]
    for row in range(ROWS):
        if copies == 1:
            parts = [x_ref[pl.ds(m * 8 + row, LAYERS, stride=24), :] for m in range(3)]
        else:
            part = x_ref[pl.ds(row, LAYERS, stride=8), :]
            part = jnp.where(iota((LAYERS, WIDE), 0) == LAYERS - 1, 0.0, part)
            parts = [part, part, part]
        parts.append(jnp.zeros((WIDE - LEVELS, WIDE), F32))
        o_ref[row] = jnp.concatenate(parts, axis=0).T


def cells_first(x, copies, *after):
    rows = x.shape[0]
    return kernel_call(
        functools.partial(table_body, copies),
        jax.ShapeDtypeStruct((ROWS, COLS, WIDE), F32),
        [pl.BlockSpec((rows, WIDE), lambda j: (0, j))] + [ANY] * len(after),
        pl.BlockSpec((ROWS, WIDE, WIDE), lambda j: (0, j, 0)),
        (x, *after),
        grid=(CHUNKS,),
    )


def copy_rows(source, target, from_row, to_row, index_of):
    def some(i, _):
        for u in range(32):
            s = i * 32 + u
            index = index_of(s)
            target[pl.ds(to_row(s, index), 1), :] = source[pl.ds(from_row(s, index), 1), :]
        return 0

    lax.fori_loop(0, SLOTS // 32, some, 0)


def pick_rows(which, place_ref, wanted_ref, table_ref, out_ref):
    def per_step(step, _):
        base = ((place_ref[1] + step) & 3) * 1024 + which * 384
        copy_rows(
            table_ref,
            out_ref,
            lambda s, index: index,
            lambda s, index: step * SLOTS + s,
            lambda s: wanted_ref[base + s],
        )
        return 0

    lax.fori_loop(0, 4, per_step, 0)


def pick_body(which, place_ref, wanted_ref, table_ref, *refs):
    pick_rows(which, place_ref, wanted_ref, table_ref, refs[-1])


MESSAGE = jax.ShapeDtypeStruct((4 * SLOTS, WIDE), F32)


def pick(which, place, wanted, table, *after):
    return kernel_call(
        functools.partial(pick_body, which),
        MESSAGE,
        [SMEM, SMEM, VMEM] + [ANY] * len(after),
        VMEM,
        (place, wanted, table, *after),
        flops=1 << 28,
    )


def pick_back_body(which, along_ref, w1, w2, w3, table, after, o1, o2, o3, s1, s2, s3, sems):
    steps = ((1, w1, o1, s1), (2, w2, o2, s2), (3, w3, o3, s3))
    for act in ("start", "finish"):
        for u, source, out, wanted in steps:

            @pl.when((along_ref[0] < SPAN) & (along_ref[0] >= u))
            def _(u=u, source=source, out=out, wanted=wanted):
                load = pltpu.make_async_copy(source, wanted, sems.at[u - 1])
                if act == "start":
                    load.start()
                else:
                    load.wait()
                    pick_rows(which, along_ref, wanted, table, out)


def pick_back(which, along, wanted, table, after):
    return kernel_call(
        functools.partial(pick_back_body, which),
        (MESSAGE,) * 3,
        [SMEM] + [ANY] * 3 + [VMEM, ANY],
        (VMEM,) * 3,
        (along, *wanted, table, after),
        scratch=[*([pltpu.SMEM((4096,), I32)] * 3), pltpu.SemaphoreType.DMA((3,))],
    )


def put_class(along_ref, kind, spot, x_ref, backs, outs, buffer, sem, relayed=None):
    def put(source):
        for step, out in enumerate(outs):
            out[spot * SLOTS : (spot + 1) * SLOTS, :] = source[step * SLOTS : (step + 1) * SLOTS, :]

    if relayed is None:
        put(x_ref)
    else:
        pl.when(along_ref[0] & 1 == 1)(lambda: put(x_ref))
        pl.when(along_ref[0] & 1 == 0)(lambda: put(relayed))
    for a in range(kind):

        @pl.when(along_ref[0] == a)
        def _(a=a):
            load = pltpu.make_async_copy(backs[kind - a - 1], buffer, sem)
            load.start()
            load.wait()
            put(buffer)


PAIR = (jax.ShapeDtypeStruct((2 * SLOTS, WIDE), F32),) * 4


def pick_join_body(which, kind, along_ref, wanted_ref, table_ref, x_ref, *refs):
    outs, (buffer, sem) = refs[-6:-2], refs[-2:]
    for step, out in enumerate(outs):
        base = ((along_ref[1] + step) & 3) * 1024 + which * 384
        copy_rows(
            table_ref, out, lambda s, index: index, lambda s, index: s, lambda s, base=base: wanted_ref[base + s]
        )
    put_class(along_ref, kind, 1, x_ref, refs[:kind], outs, buffer, sem)


def pick_join(which, kind, along, wanted, table, x, backs, *after):
    return kernel_call(
        functools.partial(pick_join_body, which, kind),
        PAIR,
        [SMEM, SMEM, VMEM, VMEM] + [ANY] * (kind + len(after)),
        (VMEM,) * 4,
        (along, wanted, table, x, *backs[:kind], *after),
        scratch=[pltpu.VMEM((4 * SLOTS, WIDE), F32), pltpu.SemaphoreType.DMA],
        flops=1 << 28,
        limit=8,
    )


def join_body(along_ref, x_ref, y_ref, relayed_ref, b1, b2, b3, *refs):
    outs, (buffer, sem) = refs[-6:-2], refs[-2:]
    put_class(along_ref, 2, 0, x_ref, (b1, b2, b3), outs, buffer, sem)
    put_class(along_ref, 3, 1, y_ref, (b1, b2, b3), outs, buffer, sem, relayed_ref)


def join(along, x, y, relayed, backs, *after):
    return kernel_call(
        join_body,
        PAIR,
        [SMEM, VMEM, VMEM, VMEM] + [ANY] * (3 + len(after)),
        (VMEM,) * 4,
        (along, x, y, relayed, *backs, *after),
        scratch=[pltpu.VMEM((4 * SLOTS, WIDE), F32), pltpu.SemaphoreType.DMA],
        flops=1 << 27,
        limit=8,
    )


def put_rows(place_ref, own_ref, xs, cells, start):
    for step, x in enumerate(xs):
        base = ((place_ref[1] - step) & 3) * 512
        copy_rows(
            x, cells, lambda s, index: start + s, lambda s, index: index, lambda s, base=base: own_ref[base + s]
        )


def load_own(which, kinds, own_any, own, sems):
    loads = [
        pltpu.make_async_copy(own_any.at[pl.ds((which * SPAN + kind) * 2048, 2048)], own[i], sems.at[i])
        for i, kind in enumerate(kinds)
    ]
    for load in loads:
        load.start()
    return loads


def place_early_body(which, kinds, place_ref, own_any, x0, x1, x2, x3, cells, own0, own1, sems):
    for i, load in enumerate(load_own(which, kinds, own_any, (own0, own1), sems)):
        load.wait()
        put_rows(place_ref, (own0, own1)[i], (x0, x1, x2, x3), cells, i * SLOTS)


def place_early(which, kinds, place, own, xs):
    return kernel_call(
        functools.partial(place_early_body, which, kinds),
        jax.ShapeDtypeStruct((CELLS + 8, WIDE), F32),
        [SMEM, ANY] + [VMEM] * 4,
        VMEM,
        (place, own, *xs),
        scratch=[*([pltpu.SMEM((2048,), I32)] * 2), pltpu.SemaphoreType.DMA((2,))],
        flops=1 << 28,
    )


def place_body(which, kinds, place_ref, own_any, cells_ref, x0, x1, x2, x3, weight_ref, out_ref, cells, own0, own1, sems):
    loads = load_own(which, kinds, own_any, (own0, own1), sems)
    cells[...] = cells_ref[...]
    for i, load in enumerate(loads):
        load.wait()
        put_rows(place_ref, (own0, own1)[i], (x0, x1, x2, x3), cells, i * SLOTS)

    def mix(i, _):
        rows = pl.ds(pl.multiple_of(i * 256, 256), 256)
        here = cells[rows, :]
        upper = pltpu.roll(here, WIDE - 1, 1)
        out_ref[rows, :] = here + weight_ref[rows, :] * (upper - here)
        return 0

    lax.fori_loop(0, CELLS // 256, mix, 0)


def place(which, kinds, where, own, cells, xs, weight):
    return kernel_call(
        functools.partial(place_body, which, kinds),
        jax.ShapeDtypeStruct((CELLS, WIDE), F32),
        [SMEM, ANY] + [VMEM] * 6,
        VMEM,
        (where, own, cells, *xs, weight),
        scratch=[
            pltpu.VMEM((CELLS + 8, WIDE), F32),
            *([pltpu.SMEM((2048,), I32)] * 2),
            pltpu.SemaphoreType.DMA((2,)),
        ],
        flops=1 << 28,
        limit=12,
    )


def pivots_body(mix_ref, drag_ref, after_ref, out_ref):
    for which in range(2):
        factor = None
        for k in range(LAYERS):
            below = None if k == 0 else mix_ref[(which * 39 + k - 1) * 8 : (which * 39 + k) * 8, :]
            above = None if k == LAYERS - 1 else mix_ref[(which * 39 + k) * 8 : (which * 39 + k + 1) * 8, :]
            diagonal = 1.0
            for term in (below, above):
                if term is not None:
                    diagonal = diagonal + term
            if k == 0 and which == 0:
                diagonal = diagonal + drag_ref[...]
            if k > 0:
                diagonal = diagonal - below * factor
            inverse = 1.0 / diagonal
            out_ref[(which * LAYERS + k) * 8 : (which * LAYERS + k + 1) * 8, :] = inverse
            if above is not None:
                factor = above * inverse


def pivots(mix, drag, after):
    return kernel_call(
        pivots_body,
        jax.ShapeDtypeStruct((2 * LAYERS * 8, COLS), F32),
        [pl.BlockSpec((2 * 39 * 8, WIDE), lambda j: (0, j)), pl.BlockSpec((8, WIDE), lambda j: (0, j)), ANY],
        pl.BlockSpec((2 * LAYERS * 8, WIDE), lambda j: (0, j)),
        (mix, drag, after),
        grid=(CHUNKS,),
    )


def layers_body(x_ref, o_ref):
    for row in range(ROWS):
        o_ref[pl.ds(row, LEVELS, stride=8), :] = x_ref[row].T[0:LEVELS, :]


def layers_first(x):
    return kernel_call(
        layers_body,
        jax.ShapeDtypeStruct((CHUNKS * LEVELS * 8, WIDE), F32),
        [pl.BlockSpec((ROWS, WIDE, WIDE), lambda j: (0, j, 0))],
        pl.BlockSpec((LEVELS * 8, WIDE), lambda j: (j, 0)),
        (x,),
        grid=(CHUNKS,),
    )


def solve_body(
    place_ref, moved_ref, up_ref, down_ref, left_ref, right_ref, lateral_ref, mix_ref, inverse_ref, stress_ref, out_ref, edge
):
    j = pl.program_id(0)
    sub, lane = iota((8, WIDE), 0), iota((8, WIDE), 1)
    size = LEVELS * 8

    def spread(source_ref):
        source = source_ref[...]
        for level in range(LEVELS):
            edge[level * 8 : level * 8 + 8, :] = jnp.broadcast_to(source[:, level : level + 1], (8, WIDE))

    @pl.when(j == 0)
    def _():
        spread(left_ref)

    @pl.when(j == CHUNKS - 1)
    def _():
        spread(right_ref)

    start = pl.multiple_of(j * size, size)
    before = pl.multiple_of(jnp.maximum(j - 1, 0) * size, size)
    after = pl.multiple_of(jnp.minimum(j + 1, CHUNKS - 1) * size, size)
    up, down = up_ref[...].T, down_ref[...].T
    lateral = lateral_ref[...]
    count = 4.0 - (
        ((place_ref[0] == 0) & (j == 0) & (lane == 0)).astype(F32)
        + ((place_ref[0] == 31) & (j == CHUNKS - 1) & (lane == WIDE - 1)).astype(F32)
        + ((place_ref[1] == 0) & (sub == 0)).astype(F32)
        + ((place_ref[1] == 3) & (sub == 7)).astype(F32)
    )
    first_chunk, last_chunk = j == 0, j == CHUNKS - 1
    for m in range(3):
        which = 0 if m < 2 else 1
        value = None
        for k in range(LAYERS):
            level = m * LAYERS + k
            at = level * 8
            here = moved_ref[pl.ds(start + at, 8), :]
            halo = edge[at : at + 8, :]
            lower = jnp.where(first_chunk, halo, moved_ref[pl.ds(before + at, 8), :])
            upper = jnp.where(last_chunk, halo, moved_ref[pl.ds(after + at, 8), :])
            west = jnp.where(lane == 0, pltpu.roll(lower, 1, 1), pltpu.roll(here, 1, 1))
            east = jnp.where(lane == WIDE - 1, pltpu.roll(upper, WIDE - 1, 1), pltpu.roll(here, WIDE - 1, 1))
            north = jnp.where(sub == 0, up[level : level + 1, :], pltpu.roll(here, 1, 0))
            south = jnp.where(sub == 7, down[level : level + 1, :], pltpu.roll(here, 7, 0))
            source = here + lateral * (((north + south) + west) + east - count * here)
            if k == LAYERS - 1 and m < 2:
                source = source + stress_ref[m * 8 : m * 8 + 8, :]
            if k > 0:
                source = source + mix_ref[(which * 39 + k - 1) * 8 : (which * 39 + k) * 8, :] * value
            value = source * inverse_ref[(which * LAYERS + k) * 8 : (which * LAYERS + k + 1) * 8, :]
            out_ref[(k * 3 + m) * 8 : (k * 3 + m + 1) * 8, :] = value
        for k in range(LAYERS - 2, -1, -1):
            rows = slice((k * 3 + m) * 8, (k * 3 + m + 1) * 8)
            factor = (
                mix_ref[(which * 39 + k) * 8 : (which * 39 + k + 1) * 8, :]
                * inverse_ref[(which * LAYERS + k) * 8 : (which * LAYERS + k + 1) * 8, :]
            )
            value = out_ref[rows, :] + factor * value
            out_ref[rows, :] = value


def solve(where, moved, up, down, left, right, lateral, mix, inverse, stress):
    def chunk(rows):
        return pl.BlockSpec((rows, WIDE), lambda j: (0, j))

    def cells(rows):
        return pl.BlockSpec((rows, WIDE), lambda j: (j, 0))

    def fixed(rows):
        return pl.BlockSpec((rows, WIDE), lambda j: (0, 0))

    return kernel_call(
        solve_body,
        jax.ShapeDtypeStruct((LEVELS * 8, COLS), F32),
        [
            SMEM,
            fixed(CHUNKS * LEVELS * 8),
            cells(WIDE),
            cells(WIDE),
            fixed(8),
            fixed(8),
            chunk(8),
            chunk(2 * 39 * 8),
            chunk(2 * LAYERS * 8),
            chunk(16),
        ],
        chunk(LEVELS * 8),
        (where, moved, up, down, left, right, lateral, mix, inverse, stress),
        grid=(CHUNKS,),
        scratch=[pltpu.VMEM((LEVELS * 8, WIDE), F32)],
        limit=14,
    )


def move(x, axis, distance, low=0, high=None):
    count = lax.axis_size(axis)
    high = count if high is None else high
    pairs = [(i, i + distance) for i in range(low, high) if 0 <= i + distance < count]
    return lax.ppermute(x, axis, pairs)


def three_up():
    count = lax.axis_size("along")
    direct, relay = [], []
    for a in range(count - 3):
        if a % 2 == 0:
            direct.append((a, a + 3))
        else:
            chip = a // 2
            between = 2 * (chip // 4 * 4 + (chip - 1) % 4)
            direct.append((a, between))
            relay.append((between, a + 3))
    return direct, relay


def body(fields, first_feet, first_fraction, second_feet, second_fraction, lateral_mix, vertical_mix, bottom_drag, surface_stress):
    along = lax.axis_index("along")
    across = lax.axis_index("across")
    where = jnp.stack([along, across]).astype(I32)

    wanted, own = kernel_call(
        slots_body,
        (jax.ShapeDtypeStruct((128, WIDE), I32),) * 2,
        [SMEM, VMEM, VMEM],
        (VMEM,) * 2,
        (where, first_feet, second_feet),
    )
    table = cells_first(fields.reshape(LEVELS * 8, COLS), 1).reshape(CELLS, WIDE)
    wanted = lax.all_to_all(wanted.reshape(4, SPAN, 8, WIDE), "across", split_axis=0, concat_axis=0, tiled=True)
    ahead = [wanted[:, 0]] + [move(wanted[:, t], "along", -t) for t in range(1, SPAN)]
    back = []
    for u in range(1, SPAN):
        payload = lax.dynamic_index_in_dim(wanted, jnp.minimum(along + u, SPAN - 1), axis=1, keepdims=False)
        pairs = [(i, i + u) for i in range(SPAN - u)]
        back.append(lax.ppermute(payload, "along", pairs))
    own = own.reshape(-1)
    ahead = [x.reshape(-1) for x in ahead]
    back = [x.reshape(-1) for x in back]

    def turn(xs):
        moved = {0: xs[0]}
        for step in (2, 1, 3):
            pairs = [(z, (z + step) % 4) for z in range(4)]
            moved[step] = lax.ppermute(xs[step], "across", pairs)
        return [moved[step] for step in range(4)]

    def fetch(which, table, weigh):
        p3 = pick(which, where, ahead[3], table, *ahead[1:], *back)
        answers = pick_back(which, where, back, table, p3)
        behind = {}
        for u in (3, 2, 1):
            pairs = [(b, b - u) for b in range(u, SPAN)]
            behind[u] = lax.ppermute(answers[u - 1], "along", pairs)
        behind = [behind[u] for u in (1, 2, 3)]
        p1 = pick(which, where, ahead[1], table, p3, *answers)
        p2 = pick(which, where, ahead[2], table, p1)
        direct, relay = three_up()
        x3 = lax.ppermute(p3, "along", direct)
        x1 = move(p1, "along", 1)
        x2 = move(p2, "along", 2)
        relayed = lax.ppermute(x3, "along", relay)
        weight, done = weigh(p2)
        joined = pick_join(which, 1, where, ahead[0], table, x1, behind, p2)
        early = turn(joined)
        late = turn(join(where, x2, x3, relayed, behind, joined[0], *done))
        cells = place_early(which, (0, 1), where, own, early)
        return place(which, (2, 3), where, own, cells, late, weight)

    mix = vertical_mix.reshape(2 * 39 * 8, COLS)
    inverse = []

    def first_weight(after):
        inverse.append(pivots(mix, bottom_drag, after))
        weight = cells_first(first_fraction.reshape(LAYERS * 8, COLS), 3, after)
        return weight.reshape(CELLS, WIDE), (weight, inverse[0])

    def second_weight(after):
        weight = cells_first(second_fraction.reshape(LAYERS * 8, COLS), 3, after)
        return weight.reshape(CELLS, WIDE), (weight,)

    middle = fetch(0, table, first_weight)
    moved = fetch(1, middle, second_weight).reshape(ROWS, COLS, WIDE)
    up = move(moved[ROWS - 1], "across", 1)
    down = move(moved[0], "across", -1)
    left = move(moved[:, COLS - 1], "along", 1)
    right = move(moved[:, 0], "along", -1)
    result = solve(
        where, layers_first(moved), up, down, left, right, lateral_mix, mix, inverse[0], surface_stress.reshape(16, COLS)
    )
    return result.reshape(LAYERS, 3, ROWS, COLS)


def solution(mesh):
    in_specs = (
        P(None, None, "across", "along"),
        P("across", "along"),
        P(None, "across", "along"),
        P("across", "along"),
        P(None, "across", "along"),
        P("across", "along"),
        P(None, None, "across", "along"),
        P("across", "along"),
        P(None, "across", "along"),
    )
    out_specs = P(None, None, "across", "along")
    return jax.shard_map(body, mesh=mesh, in_specs=in_specs, out_specs=out_specs, check_vma=False)
```

```python
import functools

import jax
import jax.numpy as jnp
from jax import lax
from jax.experimental import pallas as pl
from jax.experimental.pallas import tpu as pltpu
from jax.sharding import PartitionSpec as P


LAYERS = 40
ROWS = 8
COLS = 512
CELLS = ROWS * COLS
SLOTS = 288
SPAN = 4
WIDE = 128
CHUNKS = COLS // WIDE
LEVELS = 3 * LAYERS
F32 = jnp.float32
I32 = jnp.int32
VMEM = pl.BlockSpec(memory_space=pltpu.VMEM)
SMEM = pl.BlockSpec(memory_space=pltpu.SMEM)
ANY = pl.BlockSpec(memory_space=pl.ANY)


def iota(shape, dim):
    return lax.broadcasted_iota(I32, shape, dim)


def kernel_call(body, out_shapes, in_specs, out_specs, operands, flops=1 << 20, grid=None, scratch=(), limit=6):
    extra = {} if grid is None else {"grid": grid}
    return pl.pallas_call(
        body,
        out_shape=out_shapes,
        in_specs=in_specs,
        out_specs=out_specs,
        scratch_shapes=list(scratch),
        cost_estimate=pl.CostEstimate(flops=flops, bytes_accessed=1 << 21, transcendentals=0),
        compiler_params=pltpu.CompilerParams(vmem_limit_bytes=limit << 20),
        **extra,
    )(*operands)


def slots_body(along_ref, first_ref, second_ref, wanted_ref, own_ref):
    along = along_ref[0]
    before = (iota((COLS, COLS), 0) < iota((COLS, COLS), 1)).astype(F32).astype(jnp.bfloat16)
    partner_rows = iota((16, COLS), 0)
    slot_rows = iota((48, COLS), 0)
    lane_rows = iota((WIDE, COLS), 0)
    lane = iota((1, COLS), 1)
    wanted_ref[...] = jnp.zeros((128, WIDE), I32)
    for which, feet_ref in enumerate((first_ref, second_ref)):
        carry = jnp.zeros((16, 1), F32)
        total = jnp.zeros((192, WIDE), F32)
        for row in range(ROWS):
            feet = feet_ref[row : row + 1, :]
            global_row = feet >> 14
            column = feet & 16383
            across = global_row >> 3
            owner = column >> 9
            local = (global_row & 7) * COLS + (column & 511)
            kind = jnp.where(owner <= along, along - owner, owner)
            partner = across * SPAN + kind
            mask = partner_rows == partner
            ones = mask.astype(F32)
            prefix = jnp.dot(ones.astype(jnp.bfloat16), before, preferred_element_type=F32)
            rank = jnp.sum(jnp.where(mask, prefix + carry, 0.0), axis=0, keepdims=True).astype(I32)
            carry = carry + jnp.sum(ones, axis=1, keepdims=True)
            hit = slot_rows == partner * 3 + (rank >> 7)
            spot = (lane_rows == (rank & 127)).astype(F32).astype(jnp.bfloat16)
            own = CELLS - (row * COLS + lane)
            values = []
            for value in (local & 63, local >> 6, own & 63, own >> 6):
                values.append(jnp.where(hit, value.astype(F32), 0.0).astype(jnp.bfloat16))
            total = total + lax.dot_general(
                jnp.concatenate(values, axis=0),
                spot,
                (((1,), (1,)), ((), ())),
                preferred_element_type=F32,
            )
        whole = total.astype(I32)
        wanted = whole[0:48] + whole[48:96] * 64
        own = CELLS - (whole[96:144] + whole[144:192] * 64)
        for z in range(4):
            for kind in range(SPAN):
                partner = z * SPAN + kind
                wanted_ref[partner * 8 + which * 3 : partner * 8 + which * 3 + 3, :] = wanted[partner * 3 : partner * 3 + 3]
                place = (which * SPAN + kind) * 16 + z * 4
                own_ref[place : place + 3, :] = own[partner * 3 : partner * 3 + 3]


def table_body(copies, x_ref, *refs):
    o_ref = refs[-1]
    for row in range(ROWS):
        if copies == 1:
            parts = [x_ref[pl.ds(m * 8 + row, LAYERS, stride=24), :] for m in range(3)]
        else:
            part = x_ref[pl.ds(row, LAYERS, stride=8), :]
            part = jnp.where(iota((LAYERS, WIDE), 0) == LAYERS - 1, 0.0, part)
            parts = [part, part, part]
        parts.append(jnp.zeros((WIDE - LEVELS, WIDE), F32))
        o_ref[row] = jnp.concatenate(parts, axis=0).T


def cells_first(x, copies, *after):
    rows = x.shape[0]
    return kernel_call(
        functools.partial(table_body, copies),
        jax.ShapeDtypeStruct((ROWS, COLS, WIDE), F32),
        [pl.BlockSpec((rows, WIDE), lambda j: (0, j))] + [ANY] * len(after),
        pl.BlockSpec((ROWS, WIDE, WIDE), lambda j: (0, j, 0)),
        (x, *after),
        grid=(CHUNKS,),
    )


def copy_rows(source, target, from_row, to_row, index_of):
    def some(i, _):
        for u in range(32):
            s = i * 32 + u
            index = index_of(s)
            target[pl.ds(to_row(s, index), 1), :] = source[pl.ds(from_row(s, index), 1), :]
        return 0

    lax.fori_loop(0, SLOTS // 32, some, 0)


def pick_rows(which, place_ref, wanted_ref, table_ref, out_ref):
    def per_step(step, _):
        base = ((place_ref[1] + step) & 3) * 1024 + which * 384
        copy_rows(
            table_ref,
            out_ref,
            lambda s, index: index,
            lambda s, index: step * SLOTS + s,
            lambda s: wanted_ref[base + s],
        )
        return 0

    lax.fori_loop(0, 4, per_step, 0)


def pick_body(which, place_ref, wanted_ref, table_ref, *refs):
    pick_rows(which, place_ref, wanted_ref, table_ref, refs[-1])


MESSAGE = jax.ShapeDtypeStruct((4 * SLOTS, WIDE), F32)


def pick(which, place, wanted, table, *after):
    return kernel_call(
        functools.partial(pick_body, which),
        MESSAGE,
        [SMEM, SMEM, VMEM] + [ANY] * len(after),
        VMEM,
        (place, wanted, table, *after),
        flops=1 << 28,
    )


def pick_back_body(which, along_ref, w1, w2, w3, table, after, o1, o2, o3, s1, s2, s3, sems):
    steps = ((1, w1, o1, s1), (2, w2, o2, s2), (3, w3, o3, s3))
    for act in ("start", "finish"):
        for u, source, out, wanted in steps:

            @pl.when((along_ref[0] < SPAN) & (along_ref[0] >= u))
            def _(u=u, source=source, out=out, wanted=wanted):
                load = pltpu.make_async_copy(source, wanted, sems.at[u - 1])
                if act == "start":
                    load.start()
                else:
                    load.wait()
                    pick_rows(which, along_ref, wanted, table, out)


def pick_back(which, along, wanted, table, after):
    return kernel_call(
        functools.partial(pick_back_body, which),
        (MESSAGE,) * 3,
        [SMEM] + [ANY] * 3 + [VMEM, ANY],
        (VMEM,) * 3,
        (along, *wanted, table, after),
        scratch=[*([pltpu.SMEM((4096,), I32)] * 3), pltpu.SemaphoreType.DMA((3,))],
    )


def put_class(along_ref, kind, spot, x_ref, backs, outs, buffer, sem, relayed=None):
    def put(source):
        for step, out in enumerate(outs):
            out[spot * SLOTS : (spot + 1) * SLOTS, :] = source[step * SLOTS : (step + 1) * SLOTS, :]

    if relayed is None:
        put(x_ref)
    else:
        pl.when(along_ref[0] & 1 == 1)(lambda: put(x_ref))
        pl.when(along_ref[0] & 1 == 0)(lambda: put(relayed))
    for a in range(kind):

        @pl.when(along_ref[0] == a)
        def _(a=a):
            load = pltpu.make_async_copy(backs[kind - a - 1], buffer, sem)
            load.start()
            load.wait()
            put(buffer)


PAIR = (jax.ShapeDtypeStruct((2 * SLOTS, WIDE), F32),) * 4


def pick_join_body(which, kind, along_ref, wanted_ref, table_ref, x_ref, *refs):
    outs, (buffer, sem) = refs[-6:-2], refs[-2:]
    for step, out in enumerate(outs):
        base = ((along_ref[1] + step) & 3) * 1024 + which * 384
        copy_rows(
            table_ref, out, lambda s, index: index, lambda s, index: s, lambda s, base=base: wanted_ref[base + s]
        )
    put_class(along_ref, kind, 1, x_ref, refs[:kind], outs, buffer, sem)


def pick_join(which, kind, along, wanted, table, x, backs, *after):
    return kernel_call(
        functools.partial(pick_join_body, which, kind),
        PAIR,
        [SMEM, SMEM, VMEM, VMEM] + [ANY] * (kind + len(after)),
        (VMEM,) * 4,
        (along, wanted, table, x, *backs[:kind], *after),
        scratch=[pltpu.VMEM((4 * SLOTS, WIDE), F32), pltpu.SemaphoreType.DMA],
        flops=1 << 28,
        limit=8,
    )


def join_body(along_ref, x_ref, y_ref, relayed_ref, b1, b2, b3, *refs):
    outs, (buffer, sem) = refs[-6:-2], refs[-2:]
    put_class(along_ref, 2, 0, x_ref, (b1, b2, b3), outs, buffer, sem)
    put_class(along_ref, 3, 1, y_ref, (b1, b2, b3), outs, buffer, sem, relayed_ref)


def join(along, x, y, relayed, backs, *after):
    return kernel_call(
        join_body,
        PAIR,
        [SMEM, VMEM, VMEM, VMEM] + [ANY] * (3 + len(after)),
        (VMEM,) * 4,
        (along, x, y, relayed, *backs, *after),
        scratch=[pltpu.VMEM((4 * SLOTS, WIDE), F32), pltpu.SemaphoreType.DMA],
        flops=1 << 27,
        limit=8,
    )


def put_rows(place_ref, own_ref, xs, cells, start):
    for step, x in enumerate(xs):
        base = ((place_ref[1] - step) & 3) * 512
        copy_rows(
            x, cells, lambda s, index: start + s, lambda s, index: index, lambda s, base=base: own_ref[base + s]
        )


def load_own(which, kinds, own_any, own, sems):
    loads = [
        pltpu.make_async_copy(own_any.at[pl.ds((which * SPAN + kind) * 2048, 2048)], own[i], sems.at[i])
        for i, kind in enumerate(kinds)
    ]
    for load in loads:
        load.start()
    return loads


def place_early_body(which, kinds, place_ref, own_any, x0, x1, x2, x3, cells, own0, own1, sems):
    for i, load in enumerate(load_own(which, kinds, own_any, (own0, own1), sems)):
        load.wait()
        put_rows(place_ref, (own0, own1)[i], (x0, x1, x2, x3), cells, i * SLOTS)


def place_early(which, kinds, place, own, xs):
    return kernel_call(
        functools.partial(place_early_body, which, kinds),
        jax.ShapeDtypeStruct((CELLS + 8, WIDE), F32),
        [SMEM, ANY] + [VMEM] * 4,
        VMEM,
        (place, own, *xs),
        scratch=[*([pltpu.SMEM((2048,), I32)] * 2), pltpu.SemaphoreType.DMA((2,))],
        flops=1 << 28,
    )


def place_body(which, kinds, place_ref, own_any, cells_ref, x0, x1, x2, x3, weight_ref, out_ref, *refs):
    edges, (cells, own0, own1, sems) = refs[:-4], refs[-4:]
    loads = load_own(which, kinds, own_any, (own0, own1), sems)
    cells[...] = cells_ref[...]
    for i, load in enumerate(loads):
        load.wait()
        put_rows(place_ref, (own0, own1)[i], (x0, x1, x2, x3), cells, i * SLOTS)

    def mix(i, _):
        rows = pl.ds(pl.multiple_of(i * 256, 256), 256)
        here = cells[rows, :]
        upper = pltpu.roll(here, WIDE - 1, 1)
        out_ref[rows, :] = here + weight_ref[rows, :] * (upper - here)
        return 0

    lax.fori_loop(0, CELLS // 256, mix, 0)
    if not edges:
        return

    for even in (True, False):

        @pl.when((place_ref[1] & 1 == 0) == even)
        def _(even=even):
            high, low = edges[:2] if even else edges[1::-1]
            high[...] = out_ref[(ROWS - 1) * COLS :, :]
            low[...] = out_ref[:COLS, :]

        @pl.when((place_ref[0] & 1 == 0) == even)
        def _(even=even):
            high, low = edges[2:] if even else edges[:1:-1]
            for row in range(ROWS):
                high[row : row + 1, :] = out_ref[(row + 1) * COLS - 1 : (row + 1) * COLS, :]
                low[row : row + 1, :] = out_ref[row * COLS : row * COLS + 1, :]


EDGES = tuple(jax.ShapeDtypeStruct((n, WIDE), F32) for n in (COLS, COLS, ROWS, ROWS))


def place(which, kinds, where, own, cells, xs, weight):
    edges = EDGES if which == 1 else ()
    return kernel_call(
        functools.partial(place_body, which, kinds),
        (jax.ShapeDtypeStruct((CELLS, WIDE), F32), *edges),
        [SMEM, ANY] + [VMEM] * 6,
        (VMEM,) * (1 + len(edges)),
        (where, own, cells, *xs, weight),
        scratch=[
            pltpu.VMEM((CELLS + 8, WIDE), F32),
            *([pltpu.SMEM((2048,), I32)] * 2),
            pltpu.SemaphoreType.DMA((2,)),
        ],
        flops=1 << 28,
        limit=12,
    )


def pivots_body(mix_ref, drag_ref, after_ref, out_ref):
    for which in range(2):
        factor = None
        for k in range(LAYERS):
            below = None if k == 0 else mix_ref[(which * 39 + k - 1) * 8 : (which * 39 + k) * 8, :]
            above = None if k == LAYERS - 1 else mix_ref[(which * 39 + k) * 8 : (which * 39 + k + 1) * 8, :]
            diagonal = 1.0
            for term in (below, above):
                if term is not None:
                    diagonal = diagonal + term
            if k == 0 and which == 0:
                diagonal = diagonal + drag_ref[...]
            if k > 0:
                diagonal = diagonal - below * factor
            inverse = 1.0 / diagonal
            out_ref[(which * LAYERS + k) * 8 : (which * LAYERS + k + 1) * 8, :] = inverse
            if above is not None:
                factor = above * inverse


def pivots(mix, drag, after):
    return kernel_call(
        pivots_body,
        jax.ShapeDtypeStruct((2 * LAYERS * 8, COLS), F32),
        [pl.BlockSpec((2 * 39 * 8, WIDE), lambda j: (0, j)), pl.BlockSpec((8, WIDE), lambda j: (0, j)), ANY],
        pl.BlockSpec((2 * LAYERS * 8, WIDE), lambda j: (0, j)),
        (mix, drag, after),
        grid=(CHUNKS,),
    )


def layers_body(x_ref, o_ref):
    for row in range(ROWS):
        o_ref[pl.ds(row, LEVELS, stride=8), :] = x_ref[row].T[0:LEVELS, :]


def layers_first(x):
    return kernel_call(
        layers_body,
        jax.ShapeDtypeStruct((CHUNKS * LEVELS * 8, WIDE), F32),
        [pl.BlockSpec((ROWS, WIDE, WIDE), lambda j: (0, j, 0))],
        pl.BlockSpec((LEVELS * 8, WIDE), lambda j: (j, 0)),
        (x,),
        grid=(CHUNKS,),
    )


def solve_body(
    place_ref, moved_ref, even_row_ref, odd_row_ref, even_column_ref, odd_column_ref, lateral_ref, mix_ref, inverse_ref, stress_ref, out_ref, edge
):
    j = pl.program_id(0)
    sub, lane = iota((8, WIDE), 0), iota((8, WIDE), 1)
    size = LEVELS * 8

    even_along, even_across = place_ref[0] & 1 == 0, place_ref[1] & 1 == 0

    def spread(low):
        source = jnp.where(even_along != low, even_column_ref[...], odd_column_ref[...])
        for level in range(LEVELS):
            edge[level * 8 : level * 8 + 8, :] = jnp.broadcast_to(source[:, level : level + 1], (8, WIDE))

    @pl.when(j == 0)
    def _():
        spread(True)

    @pl.when(j == CHUNKS - 1)
    def _():
        spread(False)

    start = pl.multiple_of(j * size, size)
    before = pl.multiple_of(jnp.maximum(j - 1, 0) * size, size)
    after = pl.multiple_of(jnp.minimum(j + 1, CHUNKS - 1) * size, size)
    up = jnp.where(even_across, odd_row_ref[...], even_row_ref[...]).T
    down = jnp.where(even_across, even_row_ref[...], odd_row_ref[...]).T
    lateral = lateral_ref[...]
    count = 4.0 - (
        ((place_ref[0] == 0) & (j == 0) & (lane == 0)).astype(F32)
        + ((place_ref[0] == 31) & (j == CHUNKS - 1) & (lane == WIDE - 1)).astype(F32)
        + ((place_ref[1] == 0) & (sub == 0)).astype(F32)
        + ((place_ref[1] == 3) & (sub == 7)).astype(F32)
    )
    first_chunk, last_chunk = j == 0, j == CHUNKS - 1
    for m in range(3):
        which = 0 if m < 2 else 1
        value = None
        for k in range(LAYERS):
            level = m * LAYERS + k
            at = level * 8
            here = moved_ref[pl.ds(start + at, 8), :]
            halo = edge[at : at + 8, :]
            lower = jnp.where(first_chunk, halo, moved_ref[pl.ds(before + at, 8), :])
            upper = jnp.where(last_chunk, halo, moved_ref[pl.ds(after + at, 8), :])
            west = jnp.where(lane == 0, pltpu.roll(lower, 1, 1), pltpu.roll(here, 1, 1))
            east = jnp.where(lane == WIDE - 1, pltpu.roll(upper, WIDE - 1, 1), pltpu.roll(here, WIDE - 1, 1))
            north = jnp.where(sub == 0, up[level : level + 1, :], pltpu.roll(here, 1, 0))
            south = jnp.where(sub == 7, down[level : level + 1, :], pltpu.roll(here, 7, 0))
            source = here + lateral * (((north + south) + west) + east - count * here)
            if k == LAYERS - 1 and m < 2:
                source = source + stress_ref[m * 8 : m * 8 + 8, :]
            if k > 0:
                source = source + mix_ref[(which * 39 + k - 1) * 8 : (which * 39 + k) * 8, :] * value
            value = source * inverse_ref[(which * LAYERS + k) * 8 : (which * LAYERS + k + 1) * 8, :]
            out_ref[(k * 3 + m) * 8 : (k * 3 + m + 1) * 8, :] = value
        for k in range(LAYERS - 2, -1, -1):
            rows = slice((k * 3 + m) * 8, (k * 3 + m + 1) * 8)
            factor = (
                mix_ref[(which * 39 + k) * 8 : (which * 39 + k + 1) * 8, :]
                * inverse_ref[(which * LAYERS + k) * 8 : (which * LAYERS + k + 1) * 8, :]
            )
            value = out_ref[rows, :] + factor * value
            out_ref[rows, :] = value


def solve(where, moved, even_row, odd_row, even_column, odd_column, lateral, mix, inverse, stress):
    def chunk(rows):
        return pl.BlockSpec((rows, WIDE), lambda j: (0, j))

    def cells(rows):
        return pl.BlockSpec((rows, WIDE), lambda j: (j, 0))

    def fixed(rows):
        return pl.BlockSpec((rows, WIDE), lambda j: (0, 0))

    return kernel_call(
        solve_body,
        jax.ShapeDtypeStruct((LEVELS * 8, COLS), F32),
        [
            SMEM,
            fixed(CHUNKS * LEVELS * 8),
            cells(WIDE),
            cells(WIDE),
            fixed(8),
            fixed(8),
            chunk(8),
            chunk(2 * 39 * 8),
            chunk(2 * LAYERS * 8),
            chunk(16),
        ],
        chunk(LEVELS * 8),
        (where, moved, even_row, odd_row, even_column, odd_column, lateral, mix, inverse, stress),
        grid=(CHUNKS,),
        scratch=[pltpu.VMEM((LEVELS * 8, WIDE), F32)],
        limit=14,
    )


def move(x, axis, distance, low=0, high=None):
    count = lax.axis_size(axis)
    high = count if high is None else high
    pairs = [(i, i + distance) for i in range(low, high) if 0 <= i + distance < count]
    return lax.ppermute(x, axis, pairs)


def three_up():
    count = lax.axis_size("along")
    direct, relay = [], []
    for a in range(count - 3):
        if a % 2 == 0:
            direct.append((a, a + 3))
        else:
            chip = a // 2
            between = 2 * (chip // 4 * 4 + (chip - 1) % 4)
            direct.append((a, between))
            relay.append((between, a + 3))
    return direct, relay


def body(fields, first_feet, first_fraction, second_feet, second_fraction, lateral_mix, vertical_mix, bottom_drag, surface_stress):
    along = lax.axis_index("along")
    across = lax.axis_index("across")
    where = jnp.stack([along, across]).astype(I32)

    wanted, own = kernel_call(
        slots_body,
        (jax.ShapeDtypeStruct((128, WIDE), I32),) * 2,
        [SMEM, VMEM, VMEM],
        (VMEM,) * 2,
        (where, first_feet, second_feet),
    )
    table = cells_first(fields.reshape(LEVELS * 8, COLS), 1).reshape(CELLS, WIDE)
    wanted = lax.all_to_all(wanted.reshape(4, SPAN, 8, WIDE), "across", split_axis=0, concat_axis=0, tiled=True)
    ahead = [wanted[:, 0]] + [move(wanted[:, t], "along", -t) for t in range(1, SPAN)]
    back = []
    for u in range(1, SPAN):
        payload = lax.dynamic_index_in_dim(wanted, jnp.minimum(along + u, SPAN - 1), axis=1, keepdims=False)
        pairs = [(i, i + u) for i in range(SPAN - u)]
        back.append(lax.ppermute(payload, "along", pairs))
    own = own.reshape(-1)
    ahead = [x.reshape(-1) for x in ahead]
    back = [x.reshape(-1) for x in back]

    def turn(xs):
        moved = {0: xs[0]}
        for step in (2, 1, 3):
            pairs = [(z, (z + step) % 4) for z in range(4)]
            moved[step] = lax.ppermute(xs[step], "across", pairs)
        return [moved[step] for step in range(4)]

    def fetch(which, table, weigh):
        p3 = pick(which, where, ahead[3], table, *ahead[1:], *back)
        answers = pick_back(which, where, back, table, p3)
        behind = {}
        for u in (3, 2, 1):
            pairs = [(b, b - u) for b in range(u, SPAN)]
            behind[u] = lax.ppermute(answers[u - 1], "along", pairs)
        behind = [behind[u] for u in (1, 2, 3)]
        p1 = pick(which, where, ahead[1], table, p3, *answers)
        p2 = pick(which, where, ahead[2], table, p1)
        direct, relay = three_up()
        x3 = lax.ppermute(p3, "along", direct)
        x1 = move(p1, "along", 1)
        x2 = move(p2, "along", 2)
        relayed = lax.ppermute(x3, "along", relay)
        weight, done = weigh(p2)
        joined = pick_join(which, 1, where, ahead[0], table, x1, behind, p2)
        early = turn(joined)
        late = turn(join(where, x2, x3, relayed, behind, joined[0], *done))
        cells = place_early(which, (0, 1), where, own, early)
        return place(which, (2, 3), where, own, cells, late, weight)

    mix = vertical_mix.reshape(2 * 39 * 8, COLS)
    inverse = []

    def first_weight(after):
        inverse.append(pivots(mix, bottom_drag, after))
        weight = cells_first(first_fraction.reshape(LAYERS * 8, COLS), 3, after)
        return weight.reshape(CELLS, WIDE), (weight, inverse[0])

    def second_weight(after):
        weight = cells_first(second_fraction.reshape(LAYERS * 8, COLS), 3, after)
        return weight.reshape(CELLS, WIDE), (weight,)

    (middle,) = fetch(0, table, first_weight)
    moved, *edges = fetch(1, middle, second_weight)
    beside = []
    for axis, pair in (("across", edges[:2]), ("along", edges[2:])):
        for first, edge in enumerate(pair):
            swaps = []
            for i in range(first, lax.axis_size(axis) - 1, 2):
                swaps += [(i, i + 1), (i + 1, i)]
            beside.append(lax.ppermute(edge, axis, swaps))
    moved = layers_first(moved.reshape(ROWS, COLS, WIDE))
    result = solve(where, moved, *beside, lateral_mix, mix, inverse[0], surface_stress.reshape(16, COLS))
    return result.reshape(LAYERS, 3, ROWS, COLS)


def solution(mesh):
    in_specs = (
        P(None, None, "across", "along"),
        P("across", "along"),
        P(None, "across", "along"),
        P("across", "along"),
        P(None, "across", "along"),
        P("across", "along"),
        P(None, None, "across", "along"),
        P("across", "along"),
        P(None, "across", "along"),
    )
    out_specs = P(None, None, "across", "along")
    return jax.shard_map(body, mesh=mesh, in_specs=in_specs, out_specs=out_specs, check_vma=False)
```
